1024 devices in a mesh: node: 64 (over y, x, core), chip: 16 (over z).
Axes of the slice: x: 4, y: 8, z: 16, core: 2. Of those that a mesh axis runs over, the one named last changes fastest.
Arguments:
- momentum: float32 [1024, 128, 512], P(('node', 'chip')), may hold values from -6 to 6
- gradient: bfloat16 [1024, 128, 512], P(('node', 'chip')), may hold values from -6 to 6
- indices: int32 [1024, 16, 32], P(('node', 'chip')), may hold values from 0 to 4095, as said below
Outputs:
- new_momentum: float32 [1024, 128, 512], P(('node', 'chip'))
- update: float32 [128, 512], replicated
The draws below stay inside these ranges and needn't reach their ends.
Inputs may be any that keep to these rules, and one draw needn't show every extreme that they name: `indices`: the 32 entries of each row name distinct coefficients of their span, coefficient (k, l) being k * 64 + l.
All inputs are finite; a program needn't handle non-finite values.
Results may differ from the reference program's by a relative error of at most 0.0029.
Values may be sent and summed in bfloat16 or wider, within the bound.
A program may use at most 64 MiB of HBM per device.

```python
import math
import jax
import jax.numpy as jnp
from jax import lax

KV_WIDTH = 512
ROWS = 128
SPAN = 64
TOPK = 32
SPANS = 16
REPL = 1024


def draw_indices(key, part):
    seeds = jax.random.split(key, REPL)

    def draw_one(subkey):
        scores = jax.random.randint(subkey, (SPANS, SPAN * SPAN), 0, 2 ** 18) * (SPAN * SPAN)
        scores = scores + jnp.arange(SPAN * SPAN, dtype=jnp.int32)[None, :]
        unused, picked = lax.top_k(scores, TOPK)
        return picked.astype(jnp.int32)
    return lax.map(draw_one, seeds)


def level_of(own_key, dims, pieces, low, high):
    def one(dim, parts):
        steps = jax.random.uniform(jax.random.fold_in(jax.random.fold_in(own_key, 6), dim), (parts,), jnp.float32, low / len(pieces), high / len(pieces))
        return jnp.repeat(jnp.exp(steps), dims[dim] // parts).reshape((-1,) + (1,) * (len(dims) - dim - 1))

    gain = one(*pieces[0])
    for cut in pieces[1:]:
        gain = gain * one(*cut)
    return gain


def normal_values(rng, shape, spread, reach, pieces=(), held_as=jnp.bfloat16):
    array = jax.random.normal(rng, shape, jnp.float32) * spread
    if len(pieces) > 0:
        array = level_of(rng, shape, pieces, -0.22, 0.18) * array
    return jnp.clip(array, min=-reach, max=reach).astype(held_as)


def setup_inputs(seed: int = 0) -> dict:
    key_list = jax.random.split(jax.random.key(seed), 4)
    return {
        "momentum": normal_values(key_list[0], (REPL, ROWS, KV_WIDTH), 1.0, 6.0, ((0, 1024),), jnp.float32),
        "gradient": normal_values(key_list[1], (REPL, ROWS, KV_WIDTH), 1.0, 6.0, ((0, 1024),)),
        "indices": draw_indices(jax.random.fold_in(key_list[3], 71), 0),
    }


def dct_table(edge_len):
    orders = jnp.arange(edge_len, dtype=jnp.float32)
    wave_no = orders[:, None]
    cell_no = orders[None, :]
    factor = jnp.where(wave_no == 0.0, math.sqrt(1.0 / edge_len), math.sqrt(2.0 / edge_len))
    return factor * jnp.cos(math.pi * (2.0 * cell_no + 1.0) * wave_no / (2.0 * edge_len))

def forward(grid_field, cosines, edge_len):
    row_blocks = grid_field.shape[0] // edge_len
    col_blocks = grid_field.shape[1] // edge_len
    blocks = grid_field.reshape(row_blocks, edge_len, col_blocks, edge_len).transpose(0, 2, 1, 3)
    coeffs = jnp.einsum('kn,abnm,lm->abkl', cosines, blocks, cosines, precision=lax.Precision.HIGHEST)
    return coeffs.reshape(row_blocks * col_blocks, edge_len * edge_len)

def inverse_blocks(coeffs, cosines, edge_len):
    blocks = coeffs.reshape(coeffs.shape[0], edge_len, edge_len)
    return jnp.einsum('kn,ckl,lm->cnm', cosines, blocks, cosines, precision=lax.Precision.HIGHEST)

def place_blocks(blocks, row_count, col_count, edge_len):
    shaped = blocks.reshape(row_count // edge_len, col_count // edge_len, edge_len, edge_len)
    return shaped.transpose(0, 2, 1, 3).reshape(row_count, col_count)

def normalized(blocks):
    energy = lax.optimization_barrier(jnp.mean(blocks * blocks, axis=(1, 2), keepdims=True))
    return blocks / jnp.sqrt(energy + 1.0)

def add_entries(totals, picked, slots):
    span_ids = jnp.broadcast_to(jnp.arange(slots.shape[-2], dtype=jnp.int32)[:, None], slots.shape)
    return totals.at[span_ids, slots].add(picked.astype(jnp.float32))

def reference(momentum, gradient, indices):
    cosines = dct_table(SPAN)
    n_spans = ROWS // SPAN * (KV_WIDTH // SPAN)

    def replica_step(totals, inputs_row):
        moment, grad_row, slots = inputs_row
        blended = 0.9 * moment + grad_row.astype(jnp.float32)
        coeffs = forward(blended, cosines, SPAN)
        picked = jnp.take_along_axis(coeffs, slots, axis=1).astype(jnp.bfloat16)
        sparse = add_entries(jnp.zeros_like(coeffs), picked, slots)
        own_part = place_blocks(inverse_blocks(sparse, cosines, SPAN), ROWS, KV_WIDTH, SPAN)
        return (totals + sparse, blended - own_part)
    start_sum = jnp.zeros((n_spans, SPAN * SPAN), jnp.float32)
    totals, new_momentum = lax.scan(replica_step, start_sum, (momentum, gradient, indices))
    update = place_blocks(normalized(inverse_blocks(totals, cosines, SPAN)), ROWS, KV_WIDTH, SPAN)
    return (new_momentum, update)
```

```python
import functools

import jax
import jax.numpy as jnp
import ml_dtypes
import numpy as np
from jax import lax
from jax.experimental import pallas as pl
from jax.experimental.pallas import tpu as pltpu
from jax.sharding import PartitionSpec as P

MESH = pl.DeviceIdType.MESH
SPAN = 64
GROUP = 8
F32 = jnp.float32
BF16 = jnp.bfloat16


def cosine_tables():
    orders = np.arange(SPAN, dtype=np.float64)
    scale = np.where(orders == 0, np.sqrt(1.0 / SPAN), np.sqrt(2.0 / SPAN))[:, None]
    table = scale * np.cos(np.pi * (2 * orders[None, :] + 1) * orders[:, None] / (2 * SPAN))
    high = table.astype(ml_dtypes.bfloat16)
    low = (table - high.astype(np.float64)).astype(ml_dtypes.bfloat16)
    zero = np.zeros_like(high)
    picker = np.concatenate([high.T, low.T], axis=0)
    right = np.concatenate(
        [np.block([[part, zero], [zero, part]]) for part in (high, low)], axis=0
    )
    left = np.concatenate([high.T, high.T, low.T], axis=1)
    return picker, right, left


def split(x):
    high = x.astype(BF16)
    low = (x - high.astype(F32)).astype(BF16)
    return high, low


def mm(a, b):
    return jnp.dot(a, b, preferred_element_type=F32)


def mm_nt(a, b):
    return lax.dot_general(a, b, (((1,), (1,)), ((), ())), preferred_element_type=F32)


def far_first(n):
    return sorted(range(1, n), key=lambda d: -min(d, n - d))


def kernel(
    ys, zs, mom, grad, idx, picker_h, right_h, left_h,
    newm, upd,
    mbuf, gbuf, ibuf, picker, right, left, nbuf,
    msg, lists, zbuf, ybuf, ubuf,
    in_sem, out_sem, s1, r1, s2, r2, s3, r3, s4, r4,
):
    node = lax.axis_index("node")
    z = lax.axis_index("chip")
    p = lax.rem(node, GROUP)
    y = lax.div(node, GROUP)

    loads = [
        pltpu.make_async_copy(src, dst, in_sem.at[i])
        for i, (src, dst) in enumerate(
            [(idx.at[0], ibuf), (picker_h, picker), (mom.at[0], mbuf), (grad.at[0], gbuf),
             (right_h, right), (left_h, left)]
        )
    ]
    for load in loads:
        load.start()

    def group_peer(d):
        return (y * GROUP + lax.rem(p + d, GROUP), z)

    def y_peer(d):
        return (lax.rem(y + d, ys) * GROUP + p, z)

    def z_peer(d):
        return (node, lax.rem(z + d, zs))

    barrier = pltpu.get_barrier_semaphore()
    peers = (
        [z_peer(d) for d in far_first(zs)]
        + [y_peer(d) for d in far_first(ys)]
        + [group_peer(d) for d in far_first(GROUP)]
    )
    for peer in peers:
        pl.semaphore_signal(barrier, inc=1, device_id=peer, device_id_type=MESH)

    lane4 = lax.broadcasted_iota(jnp.int32, (4, 128), 1)
    lane64 = lax.broadcasted_iota(jnp.int32, (SPAN, 128), 1)
    row64 = lax.broadcasted_iota(jnp.int32, (SPAN, 128), 0)
    row128 = lax.broadcasted_iota(jnp.int32, (128, 128), 0)

    loads[0].wait()
    slots = jnp.concatenate([ibuf[pl.ds(j, 4, stride=4), :] for j in range(4)], axis=1)
    wave_k = slots >> 6
    wave_l = slots & 63
    hot = [(row64 == wave_k[q : q + 1]).astype(F32).astype(BF16) for q in range(4)]
    hot += [(row64 == wave_l[q : q + 1]).astype(F32).astype(BF16) for q in range(4)]
    loads[1].wait()
    waves = mm(picker[...], jnp.concatenate(hot, axis=1))
    span_of = lane64 // 32

    def spread(part):
        return jnp.concatenate(
            [jnp.where(span_of == j, part, 0.0) for j in range(4)], axis=0
        ).astype(BF16)

    cols_high = [spread(waves[0:64, 512 + 128 * q : 640 + 128 * q]) for q in range(4)]
    cols_low = [spread(waves[64:128, 512 + 128 * q : 640 + 128 * q]) for q in range(4)]
    rows_all = [
        waves[0:64, 128 * q : 128 * q + 128] + waves[64:128, 128 * q : 128 * q + 128]
        for q in range(4)
    ]

    loads[2].wait()
    loads[3].wait()
    picked = []
    for q in range(4):
        rows = slice((q // 2) * 64, (q // 2) * 64 + 64)
        cols = slice((q % 2) * 256, (q % 2) * 256 + 256)
        blended = 0.9 * mbuf[rows, cols] + gbuf[rows, cols].astype(F32)
        mbuf[rows, cols] = blended
        high, low = split(blended)
        half = mm(high, cols_high[q]) + mm(low, cols_high[q]) + mm(high, cols_low[q])
        picked.append(jnp.sum(half * rows_all[q], axis=0, keepdims=True).astype(BF16).astype(F32))

    values = jnp.concatenate(picked, axis=0)
    where = slots.astype(F32)
    even = jnp.where(lane4 < 64, values, pltpu.roll(where, 64, 1))
    odd = jnp.where(lane4 < 64, pltpu.roll(values, 64, 1), where)
    for q in range(4):
        msg[2 * q] = even[q : q + 1]
        msg[2 * q + 1] = odd[q : q + 1]
    lists[p] = msg[p]

    pl.semaphore_wait(barrier, len(peers))

    first = []
    for d in far_first(GROUP):
        peer = group_peer(d)
        copy = pltpu.make_async_remote_copy(
            src_ref=msg.at[lax.rem(p + d, GROUP)], dst_ref=lists.at[p],
            send_sem=s1.at[d - 1], recv_sem=r1.at[d - 1],
            device_id=peer, device_id_type=MESH,
        )
        copy.start()
        first.append(copy)

    stores = []
    for q in range(4):
        rows = slice((q // 2) * 64, (q // 2) * 64 + 64)
        cols = slice((q % 2) * 256, (q % 2) * 256 + 256)
        high, low = split(rows_all[q] * picked[q])
        own = mm_nt(high, cols_high[q]) + mm_nt(low, cols_high[q]) + mm_nt(high, cols_low[q])
        nbuf[rows, cols] = mbuf[rows, cols] - own
    store = pltpu.make_async_copy(nbuf, newm.at[0], out_sem.at[0])
    store.start()

    for copy in first:
        copy.wait_recv()

    got = lists[...].reshape(GROUP, 128)
    top, bottom = got[0:4], got[4:8]
    zbuf[z] = jnp.concatenate(
        [
            jnp.where(lane4 < 64, top, pltpu.roll(bottom, 64, 1)),
            jnp.where(lane4 < 64, pltpu.roll(top, 64, 1), bottom),
        ],
        axis=0,
    )
    second = []
    for d in far_first(zs):
        copy = pltpu.make_async_remote_copy(
            src_ref=zbuf.at[z], dst_ref=zbuf.at[z],
            send_sem=s2.at[d - 1], recv_sem=r2.at[d - 1],
            device_id=z_peer(d), device_id_type=MESH,
        )
        copy.start()
        second.append(copy)
    loads[4].wait()
    loads[5].wait()
    for copy in second:
        copy.wait_recv()

    def decode(step, total):
        tile = zbuf[step]
        vals = tile[0:4]
        spot = tile[4:8].astype(jnp.int32)
        at_k = spot >> 6
        at_l = (spot & 63) + ((lane4 // 32) % 2) * 64
        hot_rows, hot_cols = [], []
        for c in range(4):
            hot_rows.append((row64 == at_k[c : c + 1]).astype(F32).astype(BF16))
            hot_cols.append(jnp.where(row128 == at_l[c : c + 1], vals[c : c + 1], 0.0).astype(BF16))
        return total + mm_nt(
            jnp.concatenate(hot_rows, axis=1), jnp.concatenate(hot_cols, axis=1)
        )

    total = lax.fori_loop(0, zs, decode, jnp.zeros((SPAN, 128), F32))

    ybuf[y] = total.astype(BF16)
    third = []
    for d in far_first(ys):
        copy = pltpu.make_async_remote_copy(
            src_ref=ybuf.at[y], dst_ref=ybuf.at[y],
            send_sem=s3.at[d - 1], recv_sem=r3.at[d - 1],
            device_id=y_peer(d), device_id_type=MESH,
        )
        copy.start()
        third.append(copy)
    for copy in third:
        copy.wait_recv()
    total = ybuf[0].astype(F32)
    for i in range(1, ys):
        total = total + ybuf[i].astype(F32)

    high, low = split(total)
    half = mm(high, right[0:128]) + mm(low, right[0:128]) + mm(high, right[128:256])
    high, low = split(half)
    field = mm(left[...], jnp.concatenate([high, low, high], axis=0))
    energy = jnp.sum(total * total, axis=0, keepdims=True)
    lane1 = lax.broadcasted_iota(jnp.int32, (1, 128), 1)
    one = jnp.sum(jnp.where(lane1 < 64, energy, 0.0), axis=1, keepdims=True)
    two = jnp.sum(jnp.where(lane1 < 64, 0.0, energy), axis=1, keepdims=True)
    mean = jnp.where(lane1 < 64, one, two) * (1.0 / (SPAN * SPAN))
    ubuf[p] = (field / jnp.sqrt(mean + 1.0)).astype(BF16)

    fourth = []
    for d in far_first(GROUP):
        copy = pltpu.make_async_remote_copy(
            src_ref=ubuf.at[p], dst_ref=ubuf.at[p],
            send_sem=s4.at[d - 1], recv_sem=r4.at[d - 1],
            device_id=group_peer(d), device_id_type=MESH,
        )
        copy.start()
        fourth.append(copy)
    for copy in first + second + third:
        copy.wait_send()
    store.wait()
    for copy in fourth:
        copy.wait_recv()
    for i in range(GROUP):
        upd[(i // 4) * 64 : (i // 4) * 64 + 64, (i % 4) * 128 : (i % 4) * 128 + 128] = ubuf[
            i
        ].astype(F32)
    for copy in fourth:
        copy.wait_send()


def solution(mesh):
    zs = mesh.shape["chip"]
    ys = mesh.shape["node"] // GROUP
    tables = cosine_tables()

    def step(momentum, gradient, indices):
        anywhere = pl.BlockSpec(memory_space=pl.ANY)
        dma = pltpu.SemaphoreType.DMA
        return pl.pallas_call(
            functools.partial(kernel, ys, zs),
            out_shape=(
                jax.ShapeDtypeStruct(momentum.shape, F32),
                jax.ShapeDtypeStruct(momentum.shape[1:], F32),
            ),
            in_specs=[anywhere] * 6,
            out_specs=(anywhere, pl.BlockSpec(memory_space=pltpu.VMEM)),
            scratch_shapes=[
                pltpu.VMEM((128, 512), F32),
                pltpu.VMEM((128, 512), BF16),
                pltpu.VMEM((16, 32), jnp.int32),
                pltpu.VMEM((128, 64), BF16),
                pltpu.VMEM((256, 128), BF16),
                pltpu.VMEM((64, 192), BF16),
                pltpu.VMEM((128, 512), F32),
                pltpu.VMEM((GROUP, 1, 128), F32),
                pltpu.VMEM((GROUP, 1, 128), F32),
                pltpu.VMEM((zs, 8, 128), F32),
                pltpu.VMEM((ys, SPAN, 128), BF16),
                pltpu.VMEM((GROUP, SPAN, 128), BF16),
                dma((6,)),
                dma((1,)),
                dma((GROUP - 1,)),
                dma((GROUP - 1,)),
                dma((max(zs - 1, 1),)),
                dma((max(zs - 1, 1),)),
                dma((max(ys - 1, 1),)),
                dma((max(ys - 1, 1),)),
                dma((GROUP - 1,)),
                dma((GROUP - 1,)),
            ],
            compiler_params=pltpu.CompilerParams(collective_id=0, has_side_effects=True),
        )(momentum, gradient, indices, *(jnp.asarray(t) for t in tables))

    rows = P(("node", "chip"), None, None)
    return jax.shard_map(
        step, mesh=mesh, in_specs=(rows, rows, rows), out_specs=(rows, P()), check_vma=False
    )
```

```python
import functools

import jax
import jax.numpy as jnp
import ml_dtypes
import numpy as np
from jax import lax
from jax.experimental import pallas as pl
from jax.experimental.pallas import tpu as pltpu
from jax.sharding import PartitionSpec as P

MESH = pl.DeviceIdType.MESH
SPAN = 64
GROUP = 8
F32 = jnp.float32
BF16 = jnp.bfloat16


def cosine_tables():
    orders = np.arange(SPAN, dtype=np.float64)
    scale = np.where(orders == 0, np.sqrt(1.0 / SPAN), np.sqrt(2.0 / SPAN))[:, None]
    table = scale * np.cos(np.pi * (2 * orders[None, :] + 1) * orders[:, None] / (2 * SPAN))
    high = table.astype(ml_dtypes.bfloat16)
    low = (table - high.astype(np.float64)).astype(ml_dtypes.bfloat16)
    zero = np.zeros_like(high)
    picker = np.concatenate([high.T, low.T], axis=0)
    right = np.concatenate(
        [np.block([[part, zero], [zero, part]]) for part in (high, low)], axis=0
    )
    left = np.concatenate([high.T, high.T, low.T], axis=1)
    return picker, right, left


def split(x):
    high = x.astype(BF16)
    low = (x - high.astype(F32)).astype(BF16)
    return high, low


def mm(a, b):
    return jnp.dot(a, b, preferred_element_type=F32)


def mm_nt(a, b):
    return lax.dot_general(a, b, (((1,), (1,)), ((), ())), preferred_element_type=F32)


def far_first(n):
    return sorted(range(1, n), key=lambda d: -min(d, n - d))


def kernel(
    ys, zs, mom, grad, idx, picker_h, right_h, left_h,
    newm, upd,
    mbuf, gbuf, ibuf, picker, right, left, nbuf,
    msg, zbuf, ybuf, ubuf,
    in_sem, out_sem, s1, r1, s3, r3, s4, r4,
):
    node = lax.axis_index("node")
    z = lax.axis_index("chip")
    p = lax.rem(node, GROUP)
    y = lax.div(node, GROUP)

    loads = [
        pltpu.make_async_copy(src, dst, in_sem.at[i])
        for i, (src, dst) in enumerate(
            [(idx.at[0], ibuf), (picker_h, picker), (mom.at[0], mbuf), (grad.at[0], gbuf),
             (right_h, right), (left_h, left)]
        )
    ]
    for load in loads:
        load.start()

    def group_peer(d):
        return (y * GROUP + lax.rem(p + d, GROUP), z)

    def y_peer(d):
        return (lax.rem(y + d, ys) * GROUP + p, z)

    barrier = pltpu.get_barrier_semaphore()
    peers = [
        (y * GROUP + lax.rem(p + d, GROUP), lax.rem(z + dz, zs))
        for dz in far_first(zs)
        for d in range(GROUP)
    ]
    peers += [y_peer(d) for d in far_first(ys)] + [group_peer(d) for d in far_first(GROUP)]
    for peer in peers:
        pl.semaphore_signal(barrier, inc=1, device_id=peer, device_id_type=MESH)

    lane4 = lax.broadcasted_iota(jnp.int32, (4, 128), 1)
    lane64 = lax.broadcasted_iota(jnp.int32, (SPAN, 128), 1)
    row64 = lax.broadcasted_iota(jnp.int32, (SPAN, 128), 0)
    row128 = lax.broadcasted_iota(jnp.int32, (128, 128), 0)

    loads[0].wait()
    slots = jnp.concatenate([ibuf[pl.ds(j, 4, stride=4), :] for j in range(4)], axis=1)
    wave_k = slots >> 6
    wave_l = slots & 63
    hot = [(row64 == wave_k[q : q + 1]).astype(F32).astype(BF16) for q in range(4)]
    hot += [(row64 == wave_l[q : q + 1]).astype(F32).astype(BF16) for q in range(4)]
    loads[1].wait()
    waves = mm(picker[...], jnp.concatenate(hot, axis=1))
    span_of = lane64 // 32

    def spread(part):
        return jnp.concatenate(
            [jnp.where(span_of == j, part, 0.0) for j in range(4)], axis=0
        ).astype(BF16)

    cols_high = [spread(waves[0:64, 512 + 128 * q : 640 + 128 * q]) for q in range(4)]
    cols_low = [spread(waves[64:128, 512 + 128 * q : 640 + 128 * q]) for q in range(4)]
    rows_all = [
        waves[0:64, 128 * q : 128 * q + 128] + waves[64:128, 128 * q : 128 * q + 128]
        for q in range(4)
    ]

    loads[2].wait()
    loads[3].wait()
    picked = []
    for q in range(4):
        rows = slice((q // 2) * 64, (q // 2) * 64 + 64)
        cols = slice((q % 2) * 256, (q % 2) * 256 + 256)
        blended = 0.9 * mbuf[rows, cols] + gbuf[rows, cols].astype(F32)
        mbuf[rows, cols] = blended
        high, low = split(blended)
        half = mm(high, cols_high[q]) + mm(low, cols_high[q]) + mm(high, cols_low[q])
        picked.append(jnp.sum(half * rows_all[q], axis=0, keepdims=True).astype(BF16).astype(F32))

    values = jnp.concatenate(picked, axis=0)
    where = slots.astype(F32)
    even = jnp.where(lane4 < 64, values, pltpu.roll(where, 64, 1))
    odd = jnp.where(lane4 < 64, pltpu.roll(values, 64, 1), where)
    for q in range(4):
        msg[2 * q] = even[q : q + 1]
        msg[2 * q + 1] = odd[q : q + 1]

    pl.semaphore_wait(barrier, len(peers))

    own_list = pltpu.make_async_copy(msg.at[p], zbuf.at[z * GROUP + p], r1.at[z])
    own_list.start()
    rows_sent = [lax.rem(p + d, GROUP) for d in range(GROUP)]
    for dz in far_first(zs) + [0]:
        for d in list(range(GROUP)) if dz else far_first(GROUP):
            pltpu.make_async_remote_copy(
                src_ref=msg.at[rows_sent[d]], dst_ref=zbuf.at[z * GROUP + p],
                send_sem=s1.at[0], recv_sem=r1.at[z],
                device_id=(y * GROUP + rows_sent[d], lax.rem(z + dz, zs)), device_id_type=MESH,
            ).start()

    stores = []
    for q in range(4):
        rows = slice((q // 2) * 64, (q // 2) * 64 + 64)
        cols = slice((q % 2) * 256, (q % 2) * 256 + 256)
        high, low = split(rows_all[q] * picked[q])
        own = mm_nt(high, cols_high[q]) + mm_nt(low, cols_high[q]) + mm_nt(high, cols_low[q])
        nbuf[rows, cols] = mbuf[rows, cols] - own
    store = pltpu.make_async_copy(nbuf, newm.at[0], out_sem.at[0])
    store.start()

    total = jnp.zeros((SPAN, 128), F32)
    for step in list(range(zs // 2)) + list(range(zs - 1, zs // 2 - 1, -1)):
        slot = zbuf.at[step * GROUP : step * GROUP + GROUP]
        pltpu.make_async_copy(slot, slot, r1.at[step]).wait()
        tile = slot[...].reshape(GROUP, 128)
        top, bottom = tile[0:4], tile[4:8]
        vals = jnp.where(lane4 < 64, top, pltpu.roll(bottom, 64, 1))
        spot = jnp.where(lane4 < 64, pltpu.roll(top, 64, 1), bottom).astype(jnp.int32)
        at_k = spot >> 6
        at_l = (spot & 63) + ((lane4 // 32) % 2) * 64
        hot_rows, hot_cols = [], []
        for c in range(4):
            hot_rows.append((row64 == at_k[c : c + 1]).astype(F32).astype(BF16))
            hot_cols.append(jnp.where(row128 == at_l[c : c + 1], vals[c : c + 1], 0.0).astype(BF16))
        total = total + mm_nt(
            jnp.concatenate(hot_rows, axis=1), jnp.concatenate(hot_cols, axis=1)
        )
    loads[4].wait()
    loads[5].wait()

    ybuf[y] = total.astype(BF16)
    third = []
    for d in far_first(ys):
        copy = pltpu.make_async_remote_copy(
            src_ref=ybuf.at[y], dst_ref=ybuf.at[y],
            send_sem=s3.at[d - 1], recv_sem=r3.at[d - 1],
            device_id=y_peer(d), device_id_type=MESH,
        )
        copy.start()
        third.append(copy)
    for copy in third:
        copy.wait_recv()
    total = ybuf[0].astype(F32)
    for i in range(1, ys):
        total = total + ybuf[i].astype(F32)

    high, low = split(total)
    half = mm(high, right[0:128]) + mm(low, right[0:128]) + mm(high, right[128:256])
    high, low = split(half)
    field = mm(left[...], jnp.concatenate([high, low, high], axis=0))
    energy = jnp.sum(total * total, axis=0, keepdims=True)
    lane1 = lax.broadcasted_iota(jnp.int32, (1, 128), 1)
    one = jnp.sum(jnp.where(lane1 < 64, energy, 0.0), axis=1, keepdims=True)
    two = jnp.sum(jnp.where(lane1 < 64, 0.0, energy), axis=1, keepdims=True)
    mean = jnp.where(lane1 < 64, one, two) * (1.0 / (SPAN * SPAN))
    ubuf[p] = (field / jnp.sqrt(mean + 1.0)).astype(BF16)

    fourth = []
    for d in far_first(GROUP):
        copy = pltpu.make_async_remote_copy(
            src_ref=ubuf.at[p], dst_ref=ubuf.at[p],
            send_sem=s4.at[d - 1], recv_sem=r4.at[d - 1],
            device_id=group_peer(d), device_id_type=MESH,
        )
        copy.start()
        fourth.append(copy)
    sent = zbuf.at[0 : zs * GROUP - 1]
    pltpu.make_async_copy(sent, sent, s1.at[0]).wait()
    for copy in third:
        copy.wait_send()
    store.wait()
    for copy in fourth:
        copy.wait_recv()
    for i in range(GROUP):
        upd[(i // 4) * 64 : (i // 4) * 64 + 64, (i % 4) * 128 : (i % 4) * 128 + 128] = ubuf[
            i
        ].astype(F32)
    for copy in fourth:
        copy.wait_send()


def solution(mesh):
    zs = mesh.shape["chip"]
    ys = mesh.shape["node"] // GROUP
    tables = cosine_tables()

    def step(momentum, gradient, indices):
        anywhere = pl.BlockSpec(memory_space=pl.ANY)
        dma = pltpu.SemaphoreType.DMA
        return pl.pallas_call(
            functools.partial(kernel, ys, zs),
            out_shape=(
                jax.ShapeDtypeStruct(momentum.shape, F32),
                jax.ShapeDtypeStruct(momentum.shape[1:], F32),
            ),
            in_specs=[anywhere] * 6,
            out_specs=(anywhere, pl.BlockSpec(memory_space=pltpu.VMEM)),
            scratch_shapes=[
                pltpu.VMEM((128, 512), F32),
                pltpu.VMEM((128, 512), BF16),
                pltpu.VMEM((16, 32), jnp.int32),
                pltpu.VMEM((128, 64), BF16),
                pltpu.VMEM((256, 128), BF16),
                pltpu.VMEM((64, 192), BF16),
                pltpu.VMEM((128, 512), F32),
                pltpu.VMEM((GROUP, 1, 128), F32),
                pltpu.VMEM((zs * GROUP, 1, 128), F32),
                pltpu.VMEM((ys, SPAN, 128), BF16),
                pltpu.VMEM((GROUP, SPAN, 128), BF16),
                dma((6,)),
                dma((1,)),
                dma((1,)),
                dma((zs,)),
                dma((max(ys - 1, 1),)),
                dma((max(ys - 1, 1),)),
                dma((GROUP - 1,)),
                dma((GROUP - 1,)),
            ],
            compiler_params=pltpu.CompilerParams(collective_id=0, has_side_effects=True),
        )(momentum, gradient, indices, *(jnp.asarray(t) for t in tables))

    rows = P(("node", "chip"), None, None)
    return jax.shard_map(
        step, mesh=mesh, in_specs=(rows, rows, rows), out_specs=(rows, P()), check_vma=False
    )
```

```python
import functools

import jax
import jax.numpy as jnp
import ml_dtypes
import numpy as np
from jax import lax
from jax.experimental import pallas as pl
from jax.experimental.pallas import tpu as pltpu
from jax.sharding import PartitionSpec as P

MESH = pl.DeviceIdType.MESH
SPAN = 64
GROUP = 8
F32 = jnp.float32
BF16 = jnp.bfloat16


def cosine_tables():
    orders = np.arange(SPAN, dtype=np.float64)
    scale = np.where(orders == 0, np.sqrt(1.0 / SPAN), np.sqrt(2.0 / SPAN))[:, None]
    table = scale * np.cos(np.pi * (2 * orders[None, :] + 1) * orders[:, None] / (2 * SPAN))
    high = table.astype(ml_dtypes.bfloat16)
    low = (table - high.astype(np.float64)).astype(ml_dtypes.bfloat16)
    zero = np.zeros_like(high)
    picker = np.concatenate([high.T, low.T], axis=0)
    right = np.concatenate(
        [np.block([[part, zero], [zero, part]]) for part in (high, low)], axis=0
    )
    left = np.concatenate([high.T, high.T, low.T], axis=1)
    return picker, right, left


def split(x):
    high = x.astype(BF16)
    low = (x - high.astype(F32)).astype(BF16)
    return high, low


def mm(a, b):
    return jnp.dot(a, b, preferred_element_type=F32)


def mm_nt(a, b):
    return lax.dot_general(a, b, (((1,), (1,)), ((), ())), preferred_element_type=F32)


def far_first(n):
    return sorted(range(1, n), key=lambda d: -min(d, n - d))


def kernel(
    ys, zs, mom, grad, idx, picker_h, right_h, left_h,
    newm, upd,
    mbuf, gbuf, ibuf, picker, right, left, nbuf,
    msg, lists, zown, zbuf, ybuf, ubuf,
    in_sem, out_sem, s1, r1, s2, r2, s3, r3, s4, r4, ready,
):
    node = lax.axis_index("node")
    z = lax.axis_index("chip")
    p = lax.rem(node, GROUP)
    y = lax.div(node, GROUP)

    loads = [
        pltpu.make_async_copy(src, dst, in_sem.at[i])
        for i, (src, dst) in enumerate(
            [(idx.at[0], ibuf), (picker_h, picker), (mom.at[0], mbuf), (grad.at[0], gbuf),
             (right_h, right), (left_h, left)]
        )
    ]
    for load in loads:
        load.start()

    def group_peer(d):
        return (y * GROUP + lax.rem(p + d, GROUP), z)

    def y_peer(d):
        return (lax.rem(y + d, ys) * GROUP + p, z)

    def z_peer(d):
        return (node, lax.rem(z + d, zs))

    barrier = pltpu.get_barrier_semaphore()
    near = [group_peer(d) for d in far_first(GROUP)] + [y_peer(d) for d in far_first(ys)]
    for peer in near:
        pl.semaphore_signal(barrier, inc=1, device_id=peer, device_id_type=MESH)

    for dz in far_first(zs):

        @pl.when(z + dz < zs)
        def _():
            pl.semaphore_signal(barrier, inc=1, device_id=(node, z + dz), device_id_type=MESH)

    lane4 = lax.broadcasted_iota(jnp.int32, (4, 128), 1)
    lane64 = lax.broadcasted_iota(jnp.int32, (SPAN, 128), 1)
    row64 = lax.broadcasted_iota(jnp.int32, (SPAN, 128), 0)
    row128 = lax.broadcasted_iota(jnp.int32, (128, 128), 0)

    loads[0].wait()
    slots = jnp.concatenate([ibuf[pl.ds(j, 4, stride=4), :] for j in range(4)], axis=1)
    wave_k = slots >> 6
    wave_l = slots & 63
    hot = [(row64 == wave_k[q : q + 1]).astype(F32).astype(BF16) for q in range(4)]
    hot += [(row64 == wave_l[q : q + 1]).astype(F32).astype(BF16) for q in range(4)]
    loads[1].wait()
    waves = mm(picker[...], jnp.concatenate(hot, axis=1))
    span_of = lane64 // 32

    def spread(part):
        return jnp.concatenate(
            [jnp.where(span_of == j, part, 0.0) for j in range(4)], axis=0
        ).astype(BF16)

    cols_high = [spread(waves[0:64, 512 + 128 * q : 640 + 128 * q]) for q in range(4)]
    cols_low = [spread(waves[64:128, 512 + 128 * q : 640 + 128 * q]) for q in range(4)]
    rows_all = [
        waves[0:64, 128 * q : 128 * q + 128] + waves[64:128, 128 * q : 128 * q + 128]
        for q in range(4)
    ]

    loads[2].wait()
    loads[3].wait()
    picked = []
    for q in range(4):
        rows = slice((q // 2) * 64, (q // 2) * 64 + 64)
        cols = slice((q % 2) * 256, (q % 2) * 256 + 256)
        blended = 0.9 * mbuf[rows, cols] + gbuf[rows, cols].astype(F32)
        mbuf[rows, cols] = blended
        high, low = split(blended)
        half = mm(high, cols_high[q]) + mm(low, cols_high[q]) + mm(high, cols_low[q])
        picked.append(jnp.sum(half * rows_all[q], axis=0, keepdims=True).astype(BF16).astype(F32))

    values = jnp.concatenate(picked, axis=0)
    where = slots.astype(F32)
    even = jnp.where(lane4 < 64, values, pltpu.roll(where, 64, 1))
    odd = jnp.where(lane4 < 64, pltpu.roll(values, 64, 1), where)
    for q in range(4):
        msg[2 * q] = even[q : q + 1]
        msg[2 * q + 1] = odd[q : q + 1]
    lists[p] = msg[p]

    pl.semaphore_wait(barrier, z + len(near))

    first = []
    for d in far_first(GROUP):
        peer = group_peer(d)
        copy = pltpu.make_async_remote_copy(
            src_ref=msg.at[lax.rem(p + d, GROUP)], dst_ref=lists.at[p],
            send_sem=s1.at[d - 1], recv_sem=r1.at[d - 1],
            device_id=peer, device_id_type=MESH,
        )
        copy.start()
        first.append(copy)

    for dz in far_first(zs):

        @pl.when(z + dz >= zs)
        def _():
            pl.semaphore_signal(
                ready.at[z], inc=1, device_id=(node, z + dz - zs), device_id_type=MESH
            )

    stores = []
    for q in range(4):
        rows = slice((q // 2) * 64, (q // 2) * 64 + 64)
        cols = slice((q % 2) * 256, (q % 2) * 256 + 256)
        high, low = split(rows_all[q] * picked[q])
        own = mm_nt(high, cols_high[q]) + mm_nt(low, cols_high[q]) + mm_nt(high, cols_low[q])
        newm[0, rows, cols] = mbuf[rows, cols] - own

    for copy in first:
        copy.wait_recv()

    got = lists[...].reshape(GROUP, 128)
    top, bottom = got[0:4], got[4:8]
    zown[...] = jnp.concatenate(
        [
            jnp.where(lane4 < 64, top, pltpu.roll(bottom, 64, 1)),
            jnp.where(lane4 < 64, pltpu.roll(top, 64, 1), bottom),
        ],
        axis=0,
    )
    pltpu.make_async_copy(zown, zbuf.at[z], r2.at[z]).start()

    def send(to_z):
        pltpu.make_async_remote_copy(
            src_ref=zown, dst_ref=zbuf.at[z],
            send_sem=s2.at[0], recv_sem=r2.at[z],
            device_id=(node, to_z), device_id_type=MESH,
        ).start()

    for dz in far_first(zs):

        @pl.when(z + dz >= zs)
        def _():
            send(z + dz - zs)

    for dz in far_first(zs):

        @pl.when(z + dz < zs)
        def _():
            pl.semaphore_wait(ready.at[z + dz], 1)
            send(z + dz)

    loads[4].wait()
    loads[5].wait()

    total = jnp.zeros((SPAN, 128), F32)
    for step in list(range(zs // 2)) + list(range(zs - 1, zs // 2 - 1, -1)):
        slot = zbuf.at[step]
        pltpu.make_async_copy(slot, slot, r2.at[step]).wait()
        vals = zbuf[step, 0:4]
        spot = zbuf[step, 4:8].astype(jnp.int32)
        at_k = spot >> 6
        at_l = (spot & 63) + ((lane4 // 32) % 2) * 64
        hot_rows, hot_cols = [], []
        for c in range(4):
            hot_rows.append((row64 == at_k[c : c + 1]).astype(F32).astype(BF16))
            hot_cols.append(jnp.where(row128 == at_l[c : c + 1], vals[c : c + 1], 0.0).astype(BF16))
        total = total + mm_nt(
            jnp.concatenate(hot_rows, axis=1), jnp.concatenate(hot_cols, axis=1)
        )

    ybuf[y] = total.astype(BF16)
    third = []
    for d in far_first(ys):
        copy = pltpu.make_async_remote_copy(
            src_ref=ybuf.at[y], dst_ref=ybuf.at[y],
            send_sem=s3.at[d - 1], recv_sem=r3.at[d - 1],
            device_id=y_peer(d), device_id_type=MESH,
        )
        copy.start()
        third.append(copy)
    for copy in third:
        copy.wait_recv()
    total = ybuf[0].astype(F32)
    for i in range(1, ys):
        total = total + ybuf[i].astype(F32)

    high, low = split(total)
    half = mm(high, right[0:128]) + mm(low, right[0:128]) + mm(high, right[128:256])
    high, low = split(half)
    field = mm(left[...], jnp.concatenate([high, low, high], axis=0))
    energy = jnp.sum(total * total, axis=0, keepdims=True)
    lane1 = lax.broadcasted_iota(jnp.int32, (1, 128), 1)
    one = jnp.sum(jnp.where(lane1 < 64, energy, 0.0), axis=1, keepdims=True)
    two = jnp.sum(jnp.where(lane1 < 64, 0.0, energy), axis=1, keepdims=True)
    mean = jnp.where(lane1 < 64, one, two) * (1.0 / (SPAN * SPAN))
    ubuf[p] = (field / jnp.sqrt(mean + 1.0)).astype(BF16)

    fourth = []
    for d in far_first(GROUP):
        copy = pltpu.make_async_remote_copy(
            src_ref=ubuf.at[p], dst_ref=ubuf.at[p],
            send_sem=s4.at[d - 1], recv_sem=r4.at[d - 1],
            device_id=group_peer(d), device_id_type=MESH,
        )
        copy.start()
        fourth.append(copy)
    sent = zbuf.at[0 : zs - 1]
    pltpu.make_async_copy(sent, sent, s2.at[0]).wait()
    for copy in first + third:
        copy.wait_send()
    for copy in fourth:
        copy.wait_recv()
    for i in range(GROUP):
        upd[(i // 4) * 64 : (i // 4) * 64 + 64, (i % 4) * 128 : (i % 4) * 128 + 128] = ubuf[
            i
        ].astype(F32)
    for copy in fourth:
        copy.wait_send()


def solution(mesh):
    zs = mesh.shape["chip"]
    ys = mesh.shape["node"] // GROUP
    tables = cosine_tables()

    def step(momentum, gradient, indices):
        anywhere = pl.BlockSpec(memory_space=pl.ANY)
        dma = pltpu.SemaphoreType.DMA
        return pl.pallas_call(
            functools.partial(kernel, ys, zs),
            out_shape=(
                pltpu.VMEM(momentum.shape, F32),
                pltpu.VMEM(momentum.shape[1:], F32),
            ),
            in_specs=[anywhere] * 6,
            out_specs=(pl.BlockSpec(memory_space=pltpu.VMEM), pl.BlockSpec(memory_space=pltpu.VMEM)),
            scratch_shapes=[
                pltpu.VMEM((128, 512), F32),
                pltpu.VMEM((128, 512), BF16),
                pltpu.VMEM((16, 32), jnp.int32),
                pltpu.VMEM((128, 64), BF16),
                pltpu.VMEM((256, 128), BF16),
                pltpu.VMEM((64, 192), BF16),
                pltpu.VMEM((128, 512), F32),
                pltpu.VMEM((GROUP, 1, 128), F32),
                pltpu.VMEM((GROUP, 1, 128), F32),
                pltpu.VMEM((8, 128), F32),
                pltpu.VMEM((zs, 8, 128), F32),
                pltpu.VMEM((ys, SPAN, 128), BF16),
                pltpu.VMEM((GROUP, SPAN, 128), BF16),
                dma((6,)),
                dma((1,)),
                dma((GROUP - 1,)),
                dma((GROUP - 1,)),
                dma((1,)),
                dma((zs,)),
                dma((max(ys - 1, 1),)),
                dma((max(ys - 1, 1),)),
                dma((GROUP - 1,)),
                dma((GROUP - 1,)),
                pltpu.SemaphoreType.REGULAR((zs,)),
            ],
            compiler_params=pltpu.CompilerParams(collective_id=0, has_side_effects=True),
        )(momentum, gradient, indices, *(jnp.asarray(t) for t in tables))

    rows = P(("node", "chip"), None, None)
    return jax.shard_map(
        step, mesh=mesh, in_specs=(rows, rows, rows), out_specs=(rows, P()), check_vma=False
    )
```
